128 devices in a mesh: src: 16 (over y, z), reg: 8 (over x, core).
Axes of the slice: x: 4, y: 4, z: 4, core: 2. Of those that a mesh axis runs over, the one named last changes fastest.
Arguments:
- tiles: bfloat16 [65536, 128, 128], P(('src', 'reg')), may hold values from -0.1875 to 0.1875
- rays: float32 [8192, 128], P(('src', 'reg')), may hold values from -6 to 6
- tile_rows: int32 [65536], P(('src', 'reg')), may hold values from 0 to 63, as said below
- tile_slots: int32 [65536], P(('src', 'reg')), may hold values from 0 to 255, as said below
- tile_count: int32 [128], P(('src', 'reg')), may hold values from 256 to 512, as said below
- wanted: int32 [128, 128, 2], P(('src', 'reg')), may hold values from 0 to 255
Outputs:
- solution: float32 [32768, 128], P(('src', 'reg'))
- right_vector: float32 [32768, 128], P(('src', 'reg'))
The draws below stay inside these ranges and needn't reach their ends.
Inputs may be any that keep to these rules, and one draw needn't show every extreme that they name: `tile_rows`: non-decreasing along each device's 512 tiles. `tile_slots`: the first 256 tiles of each device name every slot once. `tile_count`: some device has all 512 tiles live.
All inputs are finite; a program needn't handle non-finite values.
Results may differ from the reference program's by a relative error of at most 0.024.
Values may be sent and summed in bfloat16 or wider, within the bound.
A program may use at most 128 MiB of HBM per device.

```python
import jax
import jax.numpy as jnp
from jax import lax

TILE = 128
BLK_DEV = 256
RB_DEV = 64
TILE_SLOTS_EACH = 512
CAP = 2
ITERS = 3
NRAYBLK = 8192
NTILE = 65536
CELL_BLOCK_SLOTS = 256
DEVICES = 128


def draw_tile_rows(key, part):
    device_list = NTILE // TILE_SLOTS_EACH
    values = jax.random.randint(key, (device_list, TILE_SLOTS_EACH), 0, RB_DEV)
    return jnp.sort(values, axis=1).reshape(-1).astype(jnp.int32)


def draw_tile_slots(key, part):
    device_list = NTILE // TILE_SLOTS_EACH
    leading_part, trailing_part = jax.random.split(jax.random.fold_in(key, 7))
    random_keys = jax.random.split(leading_part, device_list)
    running_offsets = jax.vmap(lambda iteration_index: jax.random.permutation(iteration_index, CELL_BLOCK_SLOTS))(random_keys).astype(jnp.int32)
    remaining_part = jax.random.randint(trailing_part, (device_list, TILE_SLOTS_EACH - CELL_BLOCK_SLOTS), 0, CELL_BLOCK_SLOTS).astype(jnp.int32)
    return jnp.concatenate([running_offsets, remaining_part], axis=1).reshape(-1).astype(jnp.int32)


def draw_tile_count(key, part):
    leading_part, trailing_part = jax.random.split(key)
    device_list = NTILE // TILE_SLOTS_EACH
    entry_counts = jax.random.randint(leading_part, (device_list,), CELL_BLOCK_SLOTS, TILE_SLOTS_EACH + 1)
    filled = jax.random.randint(trailing_part, (), 0, device_list)
    return entry_counts.at[filled].set(TILE_SLOTS_EACH).astype(jnp.int32)


def touch_ends(entries, stream_key, low, top_value):
    spot = [jax.random.randint(jax.random.fold_in(stream_key, axis), (), 0, length) for axis, length in enumerate(entries.shape)]
    widest = entries.shape.index(max(entries.shape))
    beside = spot[:widest] + [(spot[widest] + 1) % entries.shape[widest]] + spot[widest + 1:]
    return entries.at[tuple(spot)].set(low).at[tuple(beside)].set(top_value)


def steps_of(stream_key, extent, pieces, smallest, high):
    gain = 1.0
    for position, shards_of in pieces:
        draws = jax.random.uniform(jax.random.fold_in(jax.random.fold_in(stream_key, 6), position), (shards_of,), jnp.float32, smallest / len(pieces), high / len(pieces))
        gain = gain * jnp.repeat(jnp.exp(draws), extent[position] // shards_of).reshape((-1,) + (1,) * (len(extent) - 1 - position))
    return gain


def scatter_about(own_key, extent, spread, limit, pieces=(), kind=jnp.bfloat16):
    values = spread * jax.random.normal(own_key, extent, jnp.float32)
    if pieces:
        values = values * steps_of(own_key, extent, pieces, -0.22, 0.18)
    return jnp.clip(values, -limit, limit).astype(kind)


def setup_inputs(seed: int = 0) -> dict:
    arg_keys = jax.random.split(jax.random.key(seed), 7)
    tiles = scatter_about(arg_keys[0], (NTILE, TILE, TILE), (TILE_SLOTS_EACH * TILE // RB_DEV) ** -0.5, 0.1875, ((0, 128),))
    rays = scatter_about(arg_keys[1], (NRAYBLK, TILE), 1.0, 6.0, ((0, 128),), jnp.float32)
    tile_rows = draw_tile_rows(jax.random.fold_in(arg_keys[6], 71), 0)
    tile_slots = draw_tile_slots(jax.random.fold_in(arg_keys[6], 71), 0)
    tile_count = draw_tile_count(jax.random.fold_in(arg_keys[6], 71), 0)
    wanted = touch_ends(jax.random.randint(arg_keys[5], (DEVICES, DEVICES, CAP), 0, BLK_DEV), jax.random.fold_in(arg_keys[5], 1), 0, BLK_DEV - 1).astype(jnp.int32)
    return {"tiles": tiles, "rays": rays, "tile_rows": tile_rows, "tile_slots": tile_slots, "tile_count": tile_count, "wanted": wanted}


damping = 0.5

def column_blocks(tile_slots, wanted, blocks_dev):
    device_list = wanted.shape[0]
    cap = wanted.shape[2]
    slots = tile_slots.reshape(device_list, -1)
    owner = slots // cap
    within = slots % cap
    asking = jnp.arange(device_list, dtype=jnp.int32)[:, None]
    local = wanted[owner, asking, within]
    return (owner * blocks_dev + local).astype(jnp.int32)

def forward(tiles4, vec_bf, columns, rows, live, row_blocks):

    def one(args):
        tile_set, cols, row_ids, mask = args
        picked = vec_bf[cols].astype(jnp.float32)
        prod = jnp.einsum('tij,tj->ti', tile_set.astype(jnp.float32), picked, precision=lax.Precision.HIGHEST)
        prod = prod * mask[:, None]
        return jax.ops.segment_sum(prod, row_ids, num_segments=row_blocks)
    result = lax.map(one, (tiles4, columns, rows, live))
    return result.reshape(-1, tiles4.shape[-1])

def adjoint(tiles4, ray_bf, columns, rows, live, total_blocks):
    device_list = tiles4.shape[0]
    width = tiles4.shape[-1]
    ray_dev = ray_bf.reshape(device_list, -1, width)

    def step(total, args):
        tile_set, cols, row_ids, mask, ray_set = args
        picked = ray_set[row_ids].astype(jnp.float32)
        contrib = jnp.einsum('tij,ti->tj', tile_set.astype(jnp.float32), picked, precision=lax.Precision.HIGHEST)
        contrib = contrib * mask[:, None]
        return (total.at[cols].add(contrib), None)
    start = jnp.zeros((total_blocks, width), jnp.float32)
    total, _ = lax.scan(step, start, (tiles4, columns, rows, live, ray_dev))
    return total

def reference(tiles, rays, tile_rows, tile_slots, tile_count, wanted):
    device_list = wanted.shape[0]
    width = tiles.shape[-1]
    total_blocks = BLK_DEV * device_list
    tiles4 = tiles.reshape(device_list, -1, width, width)
    per_dev = tiles4.shape[1]
    rows = tile_rows.reshape(device_list, per_dev)
    row_blocks = rays.shape[0] // device_list
    live = (jnp.arange(per_dev, dtype=jnp.int32)[None, :] < tile_count[:, None]).astype(jnp.float32)
    columns = column_blocks(tile_slots, wanted, BLK_DEV)
    u = jnp.zeros_like(rays)
    v = jnp.zeros((total_blocks, width), jnp.float32)
    solution = jnp.zeros((total_blocks, width), jnp.float32)
    w = jnp.zeros((total_blocks, width), jnp.float32)
    uraw = rays
    vraw = v
    alpha = jnp.float32(1.0)
    phibar = jnp.float32(0.0)
    rhobar = jnp.float32(0.0)
    for step in range(ITERS + 1):
        if step > 0:
            uraw = forward(tiles4, vraw.astype(jnp.bfloat16), columns, rows, live, row_blocks) / alpha - alpha * u
        beta = jnp.sqrt(jnp.sum(uraw * uraw))
        u = uraw / beta
        grad = adjoint(tiles4, uraw.astype(jnp.bfloat16), columns, rows, live, total_blocks)
        vraw = grad / beta - beta * v
        alpha_new = jnp.sqrt(jnp.sum(vraw * vraw))
        v_new = vraw / alpha_new
        if step == 0:
            w = v_new
            phibar = beta
            rhobar = alpha_new
        else:
            rhobar1 = jnp.sqrt(rhobar * rhobar + damping * damping)
            phibar = rhobar / rhobar1 * phibar
            rho = jnp.sqrt(rhobar1 * rhobar1 + beta * beta)
            cosine = rhobar1 / rho
            sine = beta / rho
            theta = sine * alpha_new
            rhobar = -cosine * alpha_new
            phi = cosine * phibar
            phibar = sine * phibar
            solution = solution + phi / rho * w
            w = v_new - theta / rho * w
        v = v_new
        alpha = alpha_new
    scale = jnp.sqrt(jnp.float32(total_blocks * width))
    return (solution, v * scale)
```

```python
import jax
import jax.numpy as jnp
from jax import lax
from jax.experimental import pallas as pl
from jax.experimental.pallas import tpu as pltpu
from jax.sharding import Mesh
from jax.sharding import PartitionSpec as P

AXES = ("src_0", "src_1", "reg_0", "reg_1")
SIZES = (4, 4, 4, 2)
NDEV = 128
PEERS = NDEV - 1
BLK_DEV = 256
ITERS = 3
ROUNDS = 2 * ITERS + 2
NT = 512
TILE = 128
GROUP = 32
NG = NT // GROUP
MSG = 4
ROWS = NDEV * MSG
DAMPING = 0.5
BF = jnp.bfloat16
F32 = jnp.float32
MESH = pl.DeviceIdType.MESH


def peers_of(me):
    at = [
        [(me[axis] + off) % SIZES[axis] for off in range(SIZES[axis])] for axis in range(4)
    ]
    offsets = [
        (a, b, c, d) for a in range(4) for b in range(4) for c in range(4) for d in range(2)
    ]
    far = lambda o: -(min(o[0], 4 - o[0]) + min(o[1], 4 - o[1]) + min(o[2], 4 - o[2]) + o[3])
    offsets = sorted((o for o in offsets if any(o)), key=far)
    return [tuple(at[axis][o[axis]] for axis in range(4)) for o in offsets]


def index_of(place):
    return ((place[0] * 4 + place[1]) * 4 + place[2]) * 2 + place[3]


def split3(x):
    hi = x.astype(BF).astype(F32)
    mid = (x - hi).astype(BF).astype(F32)
    return hi, mid, x - hi - mid


def total(x):
    return jnp.sum(jnp.sum(x, axis=0, keepdims=True), axis=1, keepdims=True)


def split_store(ref, at, size, value):
    hi = value.astype(BF)
    ref[pl.ds(at, size), :TILE] = hi
    ref[pl.ds(at, size), TILE:] = (value - hi.astype(F32)).astype(BF)


def kernel(
    tiles_hbm, rays, idx, sol, right,
    tiles, picked, parts, s_slot, p_slot, s_row, q_row, comb, gath, uraw_r, u_r, v_r, vraw_r, w_r,
    send, recv, load_sem, send_sem, recv_sem,
):
    me = tuple(lax.axis_index(axis) for axis in AXES)
    mine = index_of(me)
    others = peers_of(me)

    def load(g):
        at = pl.ds(g * GROUP, GROUP)
        return pltpu.make_async_copy(tiles_hbm.at[at], tiles.at[at], load_sem.at[g])

    for g in range(NG):
        load(g).start()
    barrier = pltpu.get_barrier_semaphore()
    for place in others:
        pl.semaphore_signal(barrier, inc=1, device_id=place, device_id_type=MESH)

    iota = lambda shape, dim: lax.broadcasted_iota(jnp.int32, shape, dim)
    one, zero = jnp.ones((), BF), jnp.zeros((), BF)
    slots, rows, wanted, count = (idx[i : i + 1, :] for i in range(4))
    row_id = iota((ROWS, NT), 0)
    target = jnp.where(row_id % MSG < 2, (row_id // MSG) * 2 + row_id % MSG, -1)
    live_slots = jnp.where(iota((1, NT), 1) < count, slots, -2)
    hit = jnp.where(target == live_slots, 1.0, 0.0)
    s_slot[...] = hit.astype(BF)
    p_slot[...] = hit.T.astype(BF)
    hit = jnp.where(iota((64, NT), 0) == rows, 1.0, 0.0)
    s_row[...] = hit.astype(BF)
    hit = jnp.where(iota((TILE, NT), 0) == rows, 1.0, 0.0)
    q_row[...] = hit.T.astype(BF)
    hit = jnp.where(iota((BLK_DEV, ROWS), 0) == wanted, 1.0, 0.0)
    comb[...] = hit.astype(BF)
    gath[...] = hit.T.astype(BF)

    scalar_row = iota((ROWS, TILE), 0) % MSG == 2
    lane = iota((1, TILE), 1)
    scalar_mask = jnp.logical_and(scalar_row, iota((ROWS, TILE), 1) < 3)
    diag = (iota((GROUP, 16 * TILE), 0) % 16) == (iota((GROUP, 16 * TILE), 1) // TILE)

    def start_round(r, data, square):
        hi, mid, lo = split3(square)
        extra = jnp.where(lane == 0, hi, jnp.where(lane == 1, mid, jnp.where(lane == 2, lo, 0.0)))
        message = jnp.where(scalar_row, extra, data).astype(BF)
        at = pl.ds(pl.multiple_of(r * ROWS, ROWS), ROWS)
        send.reshape(ROUNDS * ROWS, TILE)[at, :] = message
        recv[r * NDEV + mine] = send[r * NDEV + mine]
        for place in others:
            pltpu.make_async_remote_copy(
                src_ref=send.at[r * NDEV + index_of(place)],
                dst_ref=recv.at[r * NDEV + mine],
                send_sem=send_sem.at[r],
                recv_sem=recv_sem.at[r],
                device_id=place,
                device_id_type=MESH,
            ).start()

    def end_round(r):
        landed = recv.at[pl.ds(r * NDEV, PEERS)]
        pltpu.make_async_copy(landed, landed, recv_sem.at[r]).wait()
        at = pl.ds(pl.multiple_of(r * ROWS, ROWS), ROWS)
        got = recv.reshape(ROUNDS * ROWS, TILE)[at, :]
        return got, total(jnp.where(scalar_mask, got.astype(F32), 0.0))

    def lhs_of(g):
        vectors = picked[pl.ds(pl.multiple_of(g * GROUP, GROUP), GROUP), :]
        return jnp.where(diag, jnp.tile(vectors, (1, 16)), zero)

    def keep(g, result):
        at = pl.multiple_of(g * GROUP, GROUP)
        split_store(parts, at, 16, result[:16, :TILE])
        split_store(parts, at + 16, 16, result[16:, TILE:])

    def adjoint_group(g):
        pair = [tiles[pl.ds(g * GROUP + 16 * h, 16)].reshape(16 * TILE, TILE) for h in range(2)]
        rhs = jnp.concatenate(pair, axis=1)
        keep(g, jnp.dot(lhs_of(g), rhs, preferred_element_type=F32))

    def forward_group(g):
        pair = []
        for h in range(2):
            block = tiles[pl.ds(g * GROUP + 16 * h, 16)]
            pair.append(jnp.concatenate([block[i] for i in range(16)], axis=1))
        rhs = jnp.concatenate(pair, axis=0)
        keep(
            g,
            lax.dot_general(
                lhs_of(g), rhs, (((1,), (1,)), ((), ())), preferred_element_type=F32
            ),
        )

    def pick_rays(uraw):
        both = jnp.concatenate([uraw, jnp.zeros_like(uraw)], axis=0).astype(BF)
        picked[...] = jnp.dot(q_row[...], both, preferred_element_type=F32).astype(BF)

    def slot_sums():
        sums = jnp.dot(s_slot[...], parts[...], preferred_element_type=F32)
        return sums[:, :TILE] + sums[:, TILE:]

    def owner_vraw(got, square, v):
        beta = jnp.sqrt(square)
        grad = jnp.dot(comb[...], got, preferred_element_type=F32)
        return beta, grad / beta - beta * v

    uraw = rays[...]
    uraw_r[...] = uraw
    v_r[...] = jnp.zeros_like(v_r)
    w_r[...] = jnp.zeros_like(w_r)
    sol[...] = jnp.zeros_like(sol)
    pick_rays(uraw)
    for g in range(NG):
        load(g).wait()
        adjoint_group(g)
    sums = slot_sums()
    pl.semaphore_wait(barrier, PEERS)
    start_round(0, sums, total(uraw * uraw))

    def iteration(k, carry):
        phibar, rhobar = carry
        got, square = end_round(2 * k)
        beta, vraw = owner_vraw(got, square, v_r[...])
        outgoing = jnp.dot(gath[...], vraw.astype(BF), preferred_element_type=F32)
        start_round(2 * k + 1, outgoing, total(vraw * vraw))
        vraw_r[...] = vraw
        u_r[...] = uraw_r[...] / beta
        got, square = end_round(2 * k + 1)
        alpha = jnp.sqrt(square)
        picked[...] = jnp.dot(p_slot[...], got, preferred_element_type=F32).astype(BF)

        def forward_step(g, c):
            forward_group(g)
            return c

        def adjoint_step(g, c):
            adjoint_group(g)
            return c

        lax.fori_loop(0, NG, forward_step, 0, unroll=4)
        both = jnp.dot(s_row[...], parts[...], preferred_element_type=F32)
        uraw = (both[:, :TILE] + both[:, TILE:]) / alpha - alpha * u_r[...]
        uraw_r[...] = uraw
        pick_rays(uraw)
        lax.fori_loop(0, NG, adjoint_step, 0, unroll=4)
        start_round(2 * k + 2, slot_sums(), total(uraw * uraw))

        first = k == 0
        v_new = vraw_r[...] / alpha
        rhobar1 = jnp.sqrt(rhobar * rhobar + DAMPING * DAMPING)
        phibar = rhobar / rhobar1 * phibar
        rho = jnp.sqrt(rhobar1 * rhobar1 + beta * beta)
        cosine = rhobar1 / rho
        sine = beta / rho
        theta = sine * alpha
        w = w_r[...]
        sol[...] += jnp.where(first, 0.0, cosine * phibar / rho) * w
        w_r[...] = v_new - jnp.where(first, 0.0, theta / rho) * w
        v_r[...] = v_new
        phibar = jnp.where(first, beta, sine * phibar)
        rhobar = jnp.where(first, alpha, -cosine * alpha)
        return phibar, rhobar

    nothing = jnp.zeros((1, 1), F32)
    phibar, rhobar = lax.fori_loop(0, ITERS, iteration, (nothing, nothing))

    got, square = end_round(2 * ITERS)
    beta, vraw = owner_vraw(got, square, v_r[...])
    start_round(2 * ITERS + 1, jnp.zeros((ROWS, TILE), F32), total(vraw * vraw))
    rhobar1 = jnp.sqrt(rhobar * rhobar + DAMPING * DAMPING)
    phibar = rhobar / rhobar1 * phibar
    rho = jnp.sqrt(rhobar1 * rhobar1 + beta * beta)
    sol[...] += rhobar1 / rho * phibar / rho * w_r[...]
    _, square = end_round(2 * ITERS + 1)
    scale = (BLK_DEV * TILE * NDEV) ** 0.5
    right[...] = vraw / jnp.sqrt(square) * scale

    def drain(r, c):
        sent = send.at[pl.ds(r * NDEV, PEERS)]
        pltpu.make_async_copy(sent, sent, send_sem.at[r]).wait()
        return c

    lax.fori_loop(0, ROUNDS, drain, 0)


def per_device(tiles, rays, tile_rows, tile_slots, tile_count, wanted):
    padded = jnp.pad(wanted[0], ((0, 0), (0, MSG - 2)), constant_values=-1).reshape(1, ROWS)
    idx = jnp.concatenate(
        [
            tile_slots.reshape(1, NT),
            tile_rows.reshape(1, NT),
            padded,
            jnp.broadcast_to(tile_count.reshape(1, 1), (5, NT)),
        ],
        axis=0,
    )
    vmem = pl.BlockSpec(memory_space=pltpu.VMEM)
    blocks = (BLK_DEV, TILE)
    return pl.pallas_call(
        kernel,
        name="lsqr",
        out_shape=(jax.ShapeDtypeStruct(blocks, F32), jax.ShapeDtypeStruct(blocks, F32)),
        in_specs=[pl.BlockSpec(memory_space=pltpu.HBM), vmem, vmem],
        out_specs=(vmem, vmem),
        scratch_shapes=[
            pltpu.VMEM((NT, TILE, TILE), BF),
            pltpu.VMEM((NT, TILE), BF),
            pltpu.VMEM((NT, 2 * TILE), BF),
            pltpu.VMEM((ROWS, NT), BF),
            pltpu.VMEM((NT, ROWS), BF),
            pltpu.VMEM((64, NT), BF),
            pltpu.VMEM((NT, TILE), BF),
            pltpu.VMEM((BLK_DEV, ROWS), BF),
            pltpu.VMEM((ROWS, BLK_DEV), BF),
            pltpu.VMEM((64, TILE), F32),
            pltpu.VMEM((64, TILE), F32),
            pltpu.VMEM(blocks, F32),
            pltpu.VMEM(blocks, F32),
            pltpu.VMEM(blocks, F32),
            pltpu.VMEM((ROUNDS * NDEV, MSG, TILE), BF),
            pltpu.VMEM((ROUNDS * NDEV, MSG, TILE), BF),
            pltpu.SemaphoreType.DMA((NG,)),
            pltpu.SemaphoreType.DMA((ROUNDS,)),
            pltpu.SemaphoreType.DMA((ROUNDS,)),
        ],
        compiler_params=pltpu.CompilerParams(
            collective_id=0, has_side_effects=True, vmem_limit_bytes=60 * 2**20
        ),
    )(tiles, rays, idx)


def solution(mesh):
    split = Mesh(mesh.devices.reshape(SIZES), AXES)
    placed = (
        P(AXES, None, None),
        P(AXES, None),
        P(AXES),
        P(AXES),
        P(AXES),
        P(AXES, None, None),
    )
    return jax.shard_map(
        per_device,
        mesh=split,
        in_specs=placed,
        out_specs=(P(AXES, None), P(AXES, None)),
        check_vma=False,
    )
```

```python
import jax
import jax.numpy as jnp
from jax import lax
from jax.experimental import pallas as pl
from jax.experimental.pallas import tpu as pltpu
from jax.sharding import Mesh
from jax.sharding import PartitionSpec as P

AXES = ("src_0", "src_1", "reg_0", "reg_1")
SIZES = (4, 4, 4, 2)
NDEV = 128
PEERS = NDEV - 1
BLK_DEV = 256
ITERS = 3
ROUNDS = 2 * ITERS + 2
NT = 512
TILE = 128
GROUP = 128
HALF = GROUP // 2
CHUNK = 32
FLIP = 32
MSG = 4
ROWS = NDEV * MSG
DAMPING = 0.5
BF = jnp.bfloat16
F32 = jnp.float32
MESH = pl.DeviceIdType.MESH


def peers_of(me):
    at = [
        [(me[axis] + off) % SIZES[axis] for off in range(SIZES[axis])] for axis in range(4)
    ]
    offsets = [
        (a, b, c, d) for a in range(4) for b in range(4) for c in range(4) for d in range(2)
    ]
    far = lambda o: -(min(o[0], 4 - o[0]) + min(o[1], 4 - o[1]) + min(o[2], 4 - o[2]) + o[3])
    offsets = sorted((o for o in offsets if any(o)), key=far)
    return [tuple(at[axis][o[axis]] for axis in range(4)) for o in offsets]


def index_of(place):
    return ((place[0] * 4 + place[1]) * 4 + place[2]) * 2 + place[3]


def total(x):
    return jnp.sum(jnp.sum(x, axis=0, keepdims=True), axis=1, keepdims=True)


def low_part(x):
    return x - x.astype(BF).astype(F32)


def kernel(
    tiles_hbm, rays_hbm, slots_hbm, rows_hbm, wanted_hbm, count_hbm,
    base_hbm, w_hbm, vraw_hbm, coef_hbm,
    tiles, flipped, rays, slots_r, rows_r, wanted_r, count_r,
    picked, parts, s_slot, p_slot, s_row, q_row, comb, gath, uraw_r, u_r, v_r, vraw_r, w_r, sol_r, coef_r,
    send, recv, load_sem, small_sem, out_sem, send_sem, recv_sem,
):
    me = tuple(lax.axis_index(axis) for axis in AXES)
    mine = index_of(me)
    others = peers_of(me)

    smalls = [
        pltpu.make_async_copy(src, dst, small_sem.at[i])
        for i, (src, dst) in enumerate(
            [
                (rows_hbm, rows_r),
                (rays_hbm, rays),
                (slots_hbm, slots_r),
                (count_hbm, count_r),
                (wanted_hbm, wanted_r),
            ]
        )
    ]

    def load(g):
        at = pl.ds(g * CHUNK, CHUNK)
        return pltpu.make_async_copy(tiles_hbm.at[at], tiles.at[at], load_sem.at[g])

    for copy in smalls:
        copy.start()
    for g in range(NT // CHUNK):
        load(g).start()
    barrier = pltpu.get_barrier_semaphore()
    for place in others:
        pl.semaphore_signal(barrier, inc=1, device_id=place, device_id_type=MESH)

    iota = lambda shape, dim: lax.broadcasted_iota(jnp.int32, shape, dim)
    zero = jnp.zeros((), BF)
    msg_id = iota((ROWS, TILE), 0) % MSG
    diag = (iota((GROUP, HALF * TILE), 0) % HALF) == (iota((GROUP, HALF * TILE), 1) // TILE)

    def one_hot(left, right):
        return jnp.where(left == right, 1.0, 0.0).astype(BF)

    def start_round(r, data, square):
        message = jnp.where(msg_id == 2, square, jnp.where(msg_id == 3, low_part(square), data))
        at = pl.ds(pl.multiple_of(r * ROWS, ROWS), ROWS)
        send.reshape(ROUNDS * ROWS, TILE)[at, :] = message.astype(BF)
        recv[r * NDEV + mine] = send[r * NDEV + mine]
        for place in others:
            pltpu.make_async_remote_copy(
                src_ref=send.at[r * NDEV + index_of(place)],
                dst_ref=recv.at[r * NDEV + mine],
                send_sem=send_sem.at[r],
                recv_sem=recv_sem.at[r],
                device_id=place,
                device_id_type=MESH,
            ).start()

    def end_round(r):
        landed = recv.at[pl.ds(r * NDEV, PEERS)]
        pltpu.make_async_copy(landed, landed, recv_sem.at[r]).wait()
        at = pl.ds(pl.multiple_of(r * ROWS, ROWS), ROWS)
        return recv.reshape(ROUNDS * ROWS, TILE)[at, :]

    def tile_group(source, g):
        at = g * GROUP
        lhs = jnp.where(diag, jnp.tile(picked[pl.ds(at, GROUP), :], (1, HALF)), zero)
        pair = [source[pl.ds(at + HALF * h, HALF)].reshape(HALF * TILE, TILE) for h in range(2)]
        result = jnp.dot(lhs, jnp.concatenate(pair, axis=1), preferred_element_type=F32)
        for h, part in enumerate((result[:HALF, :TILE], result[HALF:, TILE:])):
            where = pl.ds(at + HALF * h, HALF)
            parts[where, :TILE] = part.astype(BF)
            parts[where, TILE:] = low_part(part).astype(BF)

    def flip(first, count):
        def step(i, c):
            at = first + i * FLIP
            for j in range(FLIP):
                flipped[at + j] = tiles[at + j].T
            return c

        lax.fori_loop(0, count // FLIP, step, 0)

    def pick_rays(uraw):
        picked[...] = jnp.dot(q_row[...], uraw.astype(BF), preferred_element_type=F32).astype(BF)

    def both_halves(selector):
        sums = jnp.dot(selector, parts[...], preferred_element_type=F32)
        return sums[:, :TILE] + sums[:, TILE:]

    def owner_vraw(r, v):
        both = jnp.dot(comb[...], end_round(r), preferred_element_type=F32)
        beta = jnp.sqrt(both[BLK_DEV : BLK_DEV + 1, :])
        return beta, both[:BLK_DEV, :] / beta - beta * v

    smalls[0].wait()
    s_row[...] = one_hot(iota((64, NT), 0), rows_r[...])
    q_row[...] = one_hot(iota((64, NT), 0), rows_r[...]).astype(F32).T.astype(BF)
    smalls[1].wait()
    uraw = rays[...]
    uraw_r[...] = uraw
    pick_rays(uraw)
    smalls[2].wait()
    smalls[3].wait()
    target = jnp.where(msg_id < 2, (iota((ROWS, TILE), 0) // MSG) * 2 + msg_id, -1)
    live_slots = jnp.where(iota((1, NT), 1) < count_r[...], slots_r[...], -2)
    for j in range(NT // TILE):
        s_slot[:, j * TILE : (j + 1) * TILE] = one_hot(
            target, live_slots[:, j * TILE : (j + 1) * TILE]
        )
    coef_r[...] = jnp.zeros_like(coef_r)
    v_r[...] = jnp.zeros_like(v_r)
    w_r[...] = jnp.zeros_like(w_r)
    sol_r[...] = jnp.zeros_like(sol_r)
    square = total(uraw * uraw)
    per_group = GROUP // CHUNK
    for g in range(NT // GROUP):
        for c in range(per_group):
            load(g * per_group + c).wait()
        tile_group(tiles, g)
    sums = both_halves(s_slot[...])
    pl.semaphore_wait(barrier, PEERS)
    start_round(0, sums, square)

    smalls[4].wait()
    asked = jnp.concatenate([wanted_r[0:1, :], wanted_r[1:2, :]], axis=1)
    owned = one_hot(iota((BLK_DEV, 2 * NDEV), 0), asked)
    row = iota((ROWS, 2 * NDEV), 0)
    place_of = jnp.where(row % MSG < 2, (row % MSG) * NDEV + row // MSG, -1)
    spread = one_hot(place_of, iota((ROWS, 2 * NDEV), 1))
    nt = (((1,), (1,)), ((), ()))
    comb[:BLK_DEV, :] = lax.dot_general(
        owned, spread, nt, preferred_element_type=F32
    ).astype(BF)
    gath[...] = lax.dot_general(spread, owned, nt, preferred_element_type=F32).astype(BF)
    scalar_rows = jnp.logical_and(iota((16, ROWS), 0) == 0, iota((16, ROWS), 1) % MSG >= 2)
    scalar_rows = jnp.where(scalar_rows, 1.0, 0.0).astype(BF)
    comb[BLK_DEV:, :] = scalar_rows
    flip(0, NT // 2)

    def iteration(k, carry):
        phibar, rhobar = carry
        beta, vraw = owner_vraw(2 * k, v_r[...])
        outgoing = jnp.dot(gath[...], vraw.astype(BF), preferred_element_type=F32)
        start_round(2 * k + 1, outgoing, total(vraw * vraw))
        vraw_r[...] = vraw
        u_r[...] = uraw_r[...] / beta

        @pl.when(k == 0)
        def _():
            p_slot[:NT, :] = s_slot[...].T
            p_slot[NT:, :] = scalar_rows
            flip(NT // 2, NT // 2)

        both = jnp.dot(p_slot[...], end_round(2 * k + 1), preferred_element_type=F32)
        alpha = jnp.sqrt(both[NT : NT + 1, :])
        picked[...] = both[:NT, :].astype(BF)
        for g in range(NT // GROUP):
            tile_group(flipped, g)
        uraw = both_halves(s_row[...]) / alpha - alpha * u_r[...]
        uraw_r[...] = uraw
        pick_rays(uraw)
        for g in range(NT // GROUP):
            tile_group(tiles, g)
        start_round(2 * k + 2, both_halves(s_slot[...]), total(uraw * uraw))

        first = k == 0
        v_new = vraw_r[...] / alpha
        rhobar1 = jnp.sqrt(rhobar * rhobar + DAMPING * DAMPING)
        phibar = rhobar / rhobar1 * phibar
        rho = jnp.sqrt(rhobar1 * rhobar1 + beta * beta)
        cosine = rhobar1 / rho
        sine = beta / rho
        theta = sine * alpha
        w = w_r[...]
        sol_r[...] += jnp.where(first, 0.0, cosine * phibar / rho) * w
        w_r[...] = v_new - jnp.where(first, 0.0, theta / rho) * w
        v_r[...] = v_new
        phibar = jnp.where(first, beta, sine * phibar)
        rhobar = jnp.where(first, alpha, -cosine * alpha)
        return phibar, rhobar

    nothing = jnp.zeros((1, TILE), F32)
    phibar, rhobar = lax.fori_loop(0, ITERS, iteration, (nothing, nothing))

    outs = [
        pltpu.make_async_copy(src, dst, out_sem.at[i])
        for i, (src, dst) in enumerate(
            [(sol_r, base_hbm), (w_r, w_hbm), (vraw_r, vraw_hbm), (coef_r, coef_hbm)]
        )
    ]
    outs[0].start()
    outs[1].start()
    beta, vraw = owner_vraw(2 * ITERS, v_r[...])
    start_round(2 * ITERS + 1, jnp.zeros((ROWS, TILE), F32), total(vraw * vraw))
    vraw_r[...] = vraw
    outs[2].start()
    rhobar1 = jnp.sqrt(rhobar * rhobar + DAMPING * DAMPING)
    phibar = rhobar / rhobar1 * phibar
    rho = jnp.sqrt(rhobar1 * rhobar1 + beta * beta)
    coef_r[0:1, :] = rhobar1 / rho * phibar / rho

    def drain(r, c):
        sent = send.at[pl.ds(r * NDEV, PEERS)]
        pltpu.make_async_copy(sent, sent, send_sem.at[r]).wait()
        return c

    lax.fori_loop(0, ROUNDS, drain, 0)
    for copy in outs[:3]:
        copy.wait()
    both = jnp.dot(comb[BLK_DEV:, :], end_round(2 * ITERS + 1), preferred_element_type=F32)
    coef_r[1:2, :] = (BLK_DEV * TILE * NDEV) ** 0.5 / jnp.sqrt(both[0:1, :])
    outs[3].start()
    outs[3].wait()


def per_device(tiles, rays, tile_rows, tile_slots, tile_count, wanted):
    hbm = pl.BlockSpec(memory_space=pltpu.HBM)
    blocks = (BLK_DEV, TILE)
    shapes = [blocks, blocks, blocks, (8, TILE)]
    base, w, vraw, coef = pl.pallas_call(
        kernel,
        name="lsqr",
        out_shape=[jax.ShapeDtypeStruct(shape, F32) for shape in shapes],
        in_specs=[hbm] * 6,
        out_specs=[hbm] * 4,
        scratch_shapes=[
            pltpu.VMEM((NT, TILE, TILE), BF),
            pltpu.VMEM((NT, TILE, TILE), BF),
            pltpu.VMEM((64, TILE), F32),
            pltpu.VMEM((1, NT), jnp.int32),
            pltpu.VMEM((1, NT), jnp.int32),
            pltpu.VMEM((2, NDEV), jnp.int32),
            pltpu.VMEM((1, 1), jnp.int32),
            pltpu.VMEM((NT, TILE), BF),
            pltpu.VMEM((NT, 2 * TILE), BF),
            pltpu.VMEM((ROWS, NT), BF),
            pltpu.VMEM((NT + 16, ROWS), BF),
            pltpu.VMEM((64, NT), BF),
            pltpu.VMEM((NT, 64), BF),
            pltpu.VMEM((BLK_DEV + 16, ROWS), BF),
            pltpu.VMEM((ROWS, BLK_DEV), BF),
            pltpu.VMEM((64, TILE), F32),
            pltpu.VMEM((64, TILE), F32),
            pltpu.VMEM(blocks, F32),
            pltpu.VMEM(blocks, F32),
            pltpu.VMEM(blocks, F32),
            pltpu.VMEM(blocks, F32),
            pltpu.VMEM((8, TILE), F32),
            pltpu.VMEM((ROUNDS * NDEV, MSG, TILE), BF),
            pltpu.VMEM((ROUNDS * NDEV, MSG, TILE), BF),
            pltpu.SemaphoreType.DMA((NT // CHUNK,)),
            pltpu.SemaphoreType.DMA((5,)),
            pltpu.SemaphoreType.DMA((4,)),
            pltpu.SemaphoreType.DMA((ROUNDS,)),
            pltpu.SemaphoreType.DMA((ROUNDS,)),
        ],
        compiler_params=pltpu.CompilerParams(
            collective_id=0, has_side_effects=True, vmem_limit_bytes=60 * 2**20
        ),
    )(
        tiles,
        rays,
        tile_slots.reshape(1, NT),
        tile_rows.reshape(1, NT),
        wanted[0].T,
        tile_count.reshape(1, 1),
    )
    return base + coef[0:1, :] * w, vraw * coef[1:2, :]


def solution(mesh):
    split = Mesh(mesh.devices.reshape(SIZES), AXES)
    placed = (
        P(AXES, None, None),
        P(AXES, None),
        P(AXES),
        P(AXES),
        P(AXES),
        P(AXES, None, None),
    )
    return jax.shard_map(
        per_device,
        mesh=split,
        in_specs=placed,
        out_specs=(P(AXES, None), P(AXES, None)),
        check_vma=False,
    )
```

```python
import jax
import jax.numpy as jnp
from jax import lax
from jax.experimental import pallas as pl
from jax.experimental.pallas import tpu as pltpu
from jax.sharding import Mesh
from jax.sharding import PartitionSpec as P

AXES = ("src_0", "src_1", "reg_0", "reg_1")
SIZES = (4, 4, 4, 2)
NDEV = 128
PEERS = NDEV - 1
BLK_DEV = 256
ITERS = 3
ROUNDS = 2 * ITERS + 2
NT = 512
TILE = 128
GROUP = 128
HALF = GROUP // 2
CHUNK = 32
FLIP = 32
MSG = 4
ROWS = NDEV * MSG
DAMPING = 0.5
BF = jnp.bfloat16
F32 = jnp.float32
MESH = pl.DeviceIdType.MESH


def peers_of(me):
    at = [
        [(me[axis] + off) % SIZES[axis] for off in range(SIZES[axis])] for axis in range(4)
    ]
    offsets = [
        (a, b, c, d) for a in range(4) for b in range(4) for c in range(4) for d in range(2)
    ]
    far = lambda o: -(min(o[0], 4 - o[0]) + min(o[1], 4 - o[1]) + min(o[2], 4 - o[2]) + o[3])
    offsets = sorted((o for o in offsets if any(o)), key=far)
    return [tuple(at[axis][o[axis]] for axis in range(4)) for o in offsets]


def index_of(place):
    return ((place[0] * 4 + place[1]) * 4 + place[2]) * 2 + place[3]


def total(x):
    return jnp.sum(jnp.sum(x, axis=0, keepdims=True), axis=1, keepdims=True)


def low_part(x):
    return x - x.astype(BF).astype(F32)


def kernel(
    tiles_hbm, rays_hbm, slots_hbm, rows_hbm, wanted_hbm, count_hbm,
    base_hbm, w_hbm, vraw_hbm, csol_hbm, cright_hbm,
    tiles, flipped, rays, slots_r, rows_r, wanted_r, count_r,
    picked, parts, s_slot, p_slot, s_row, q_row, comb, gath, uraw_r, u_r, v_r, vraw_r, w_r, sol_r, csol_r, cright_r,
    send, recv, load_sem, small_sem, out_sem, send_sem, recv_sem,
):
    me = tuple(lax.axis_index(axis) for axis in AXES)
    mine = index_of(me)
    others = peers_of(me)

    smalls = [
        pltpu.make_async_copy(src, dst, small_sem.at[i])
        for i, (src, dst) in enumerate(
            [
                (rows_hbm, rows_r),
                (rays_hbm, rays),
                (slots_hbm, slots_r),
                (count_hbm, count_r),
                (wanted_hbm, wanted_r),
            ]
        )
    ]

    def load(g):
        at = pl.ds(g * CHUNK, CHUNK)
        return pltpu.make_async_copy(tiles_hbm.at[at], tiles.at[at], load_sem.at[g])

    for copy in smalls:
        copy.start()
    for g in range(NT // CHUNK):
        load(g).start()
    barrier = pltpu.get_barrier_semaphore()
    for place in others:
        pl.semaphore_signal(barrier, inc=1, device_id=place, device_id_type=MESH)

    iota = lambda shape, dim: lax.broadcasted_iota(jnp.int32, shape, dim)
    zero = jnp.zeros((), BF)
    msg_id = iota((ROWS, TILE), 0) % MSG
    diag = (iota((GROUP, HALF * TILE), 0) % HALF) == (iota((GROUP, HALF * TILE), 1) // TILE)

    def one_hot(left, right):
        return jnp.where(left == right, 1.0, 0.0).astype(BF)

    def start_round(r, data, square):
        message = jnp.where(msg_id == 2, square, jnp.where(msg_id == 3, low_part(square), data))
        at = pl.ds(pl.multiple_of(r * ROWS, ROWS), ROWS)
        send.reshape(ROUNDS * ROWS, TILE)[at, :] = message.astype(BF)
        recv[r * NDEV + mine] = send[r * NDEV + mine]
        for place in others:
            pltpu.make_async_remote_copy(
                src_ref=send.at[r * NDEV + index_of(place)],
                dst_ref=recv.at[r * NDEV + mine],
                send_sem=send_sem.at[r],
                recv_sem=recv_sem.at[r],
                device_id=place,
                device_id_type=MESH,
            ).start()

    def end_round(r):
        landed = recv.at[pl.ds(r * NDEV, PEERS)]
        pltpu.make_async_copy(landed, landed, recv_sem.at[r]).wait()
        at = pl.ds(pl.multiple_of(r * ROWS, ROWS), ROWS)
        return recv.reshape(ROUNDS * ROWS, TILE)[at, :]

    def tile_group(source, g):
        at = g * GROUP
        lhs = jnp.where(diag, jnp.tile(picked[pl.ds(at, GROUP), :], (1, HALF)), zero)
        pair = [source[pl.ds(at + HALF * h, HALF)].reshape(HALF * TILE, TILE) for h in range(2)]
        result = jnp.dot(lhs, jnp.concatenate(pair, axis=1), preferred_element_type=F32)
        for h, part in enumerate((result[:HALF, :TILE], result[HALF:, TILE:])):
            where = pl.ds(at + HALF * h, HALF)
            parts[where, :TILE] = part.astype(BF)
            parts[where, TILE:] = low_part(part).astype(BF)

    def flip(first, count):
        def step(i, c):
            at = first + i * FLIP
            for j in range(FLIP):
                flipped[at + j] = tiles[at + j].T
            return c

        lax.fori_loop(0, count // FLIP, step, 0)

    def pick_rays(uraw):
        picked[...] = jnp.dot(q_row[...], uraw.astype(BF), preferred_element_type=F32).astype(BF)

    def both_halves(selector):
        sums = jnp.dot(selector, parts[...], preferred_element_type=F32)
        return sums[:, :TILE] + sums[:, TILE:]

    def owner_vraw(r, v):
        both = jnp.dot(comb[...], end_round(r), preferred_element_type=F32)
        beta = jnp.sqrt(both[BLK_DEV : BLK_DEV + 1, :])
        return beta, both[:BLK_DEV, :] / beta - beta * v

    smalls[0].wait()
    s_row[...] = one_hot(iota((64, NT), 0), rows_r[...])
    q_row[...] = one_hot(iota((64, NT), 0), rows_r[...]).astype(F32).T.astype(BF)
    smalls[1].wait()
    uraw = rays[...]
    uraw_r[...] = uraw
    pick_rays(uraw)
    smalls[2].wait()
    smalls[3].wait()
    target = jnp.where(msg_id < 2, (iota((ROWS, TILE), 0) // MSG) * 2 + msg_id, -1)
    live_slots = jnp.where(iota((1, NT), 1) < count_r[...], slots_r[...], -2)
    for j in range(NT // TILE):
        s_slot[:, j * TILE : (j + 1) * TILE] = one_hot(
            target, live_slots[:, j * TILE : (j + 1) * TILE]
        )
    v_r[...] = jnp.zeros_like(v_r)
    w_r[...] = jnp.zeros_like(w_r)
    sol_r[...] = jnp.zeros_like(sol_r)
    square = total(uraw * uraw)
    per_group = GROUP // CHUNK
    for g in range(NT // GROUP):
        for c in range(per_group):
            load(g * per_group + c).wait()
        tile_group(tiles, g)
    sums = both_halves(s_slot[...])
    pl.semaphore_wait(barrier, PEERS)
    start_round(0, sums, square)

    smalls[4].wait()
    asked = jnp.concatenate([wanted_r[0:1, :], wanted_r[1:2, :]], axis=1)
    owned = one_hot(iota((BLK_DEV, 2 * NDEV), 0), asked)
    row = iota((ROWS, 2 * NDEV), 0)
    place_of = jnp.where(row % MSG < 2, (row % MSG) * NDEV + row // MSG, -1)
    spread = one_hot(place_of, iota((ROWS, 2 * NDEV), 1))
    nt = (((1,), (1,)), ((), ()))
    comb[:BLK_DEV, :] = lax.dot_general(
        owned, spread, nt, preferred_element_type=F32
    ).astype(BF)
    gath[...] = lax.dot_general(spread, owned, nt, preferred_element_type=F32).astype(BF)
    scalar_rows = jnp.logical_and(iota((16, ROWS), 0) == 0, iota((16, ROWS), 1) % MSG >= 2)
    scalar_rows = jnp.where(scalar_rows, 1.0, 0.0).astype(BF)
    comb[BLK_DEV:, :] = scalar_rows
    flip(0, NT // 2)

    def iteration(k, carry):
        phibar, rhobar = carry
        beta, vraw = owner_vraw(2 * k, v_r[...])
        outgoing = jnp.dot(gath[...], vraw.astype(BF), preferred_element_type=F32)
        start_round(2 * k + 1, outgoing, total(vraw * vraw))
        vraw_r[...] = vraw
        u_r[...] = uraw_r[...] / beta

        @pl.when(k == 0)
        def _():
            p_slot[:NT, :] = s_slot[...].T
            p_slot[NT:, :] = scalar_rows
            flip(NT // 2, NT // 2)

        both = jnp.dot(p_slot[...], end_round(2 * k + 1), preferred_element_type=F32)
        alpha = jnp.sqrt(both[NT : NT + 1, :])
        picked[...] = both[:NT, :].astype(BF)
        for g in range(NT // GROUP):
            tile_group(flipped, g)
        uraw = both_halves(s_row[...]) / alpha - alpha * u_r[...]
        uraw_r[...] = uraw
        pick_rays(uraw)
        for g in range(NT // GROUP):
            tile_group(tiles, g)
        start_round(2 * k + 2, both_halves(s_slot[...]), total(uraw * uraw))

        first = k == 0
        v_new = vraw_r[...] / alpha
        rhobar1 = jnp.sqrt(rhobar * rhobar + DAMPING * DAMPING)
        phibar = rhobar / rhobar1 * phibar
        rho = jnp.sqrt(rhobar1 * rhobar1 + beta * beta)
        cosine = rhobar1 / rho
        sine = beta / rho
        theta = sine * alpha
        w = w_r[...]
        sol_r[...] += jnp.where(first, 0.0, cosine * phibar / rho) * w
        w_r[...] = v_new - jnp.where(first, 0.0, theta / rho) * w
        v_r[...] = v_new
        phibar = jnp.where(first, beta, sine * phibar)
        rhobar = jnp.where(first, alpha, -cosine * alpha)
        return phibar, rhobar

    nothing = jnp.zeros((1, TILE), F32)
    phibar, rhobar = lax.fori_loop(0, ITERS, iteration, (nothing, nothing))

    outs = [
        pltpu.make_async_copy(src, dst, out_sem.at[i])
        for i, (src, dst) in enumerate(
            [(sol_r, base_hbm), (w_r, w_hbm), (vraw_r, vraw_hbm), (csol_r, csol_hbm), (cright_r, cright_hbm)]
        )
    ]
    outs[0].start()
    outs[1].start()
    beta, vraw = owner_vraw(2 * ITERS, v_r[...])
    start_round(2 * ITERS + 1, jnp.zeros((ROWS, TILE), F32), total(vraw * vraw))
    vraw_r[...] = vraw
    outs[2].start()
    rhobar1 = jnp.sqrt(rhobar * rhobar + DAMPING * DAMPING)
    phibar = rhobar / rhobar1 * phibar
    rho = jnp.sqrt(rhobar1 * rhobar1 + beta * beta)
    csol_r[...] = rhobar1 / rho * phibar / rho
    outs[3].start()

    def drain(r, c):
        sent = send.at[pl.ds(r * NDEV, PEERS)]
        pltpu.make_async_copy(sent, sent, send_sem.at[r]).wait()
        return c

    lax.fori_loop(0, ROUNDS, drain, 0)
    for copy in outs[:4]:
        copy.wait()
    both = jnp.dot(comb[BLK_DEV:, :], end_round(2 * ITERS + 1), preferred_element_type=F32)
    cright_r[...] = (BLK_DEV * TILE * NDEV) ** 0.5 / jnp.sqrt(both[0:1, :])
    outs[4].start()
    outs[4].wait()


def per_device(tiles, rays, tile_rows, tile_slots, tile_count, wanted):
    hbm = pl.BlockSpec(memory_space=pltpu.HBM)
    blocks = (BLK_DEV, TILE)
    shapes = [blocks, blocks, blocks, (1, TILE), (1, TILE)]
    base, w, vraw, coef_sol, coef_right = pl.pallas_call(
        kernel,
        name="lsqr",
        out_shape=[jax.ShapeDtypeStruct(shape, F32) for shape in shapes],
        in_specs=[hbm] * 6,
        out_specs=[hbm] * 5,
        scratch_shapes=[
            pltpu.VMEM((NT, TILE, TILE), BF),
            pltpu.VMEM((NT, TILE, TILE), BF),
            pltpu.VMEM((64, TILE), F32),
            pltpu.VMEM((1, NT), jnp.int32),
            pltpu.VMEM((1, NT), jnp.int32),
            pltpu.VMEM((2, NDEV), jnp.int32),
            pltpu.VMEM((1, 1), jnp.int32),
            pltpu.VMEM((NT, TILE), BF),
            pltpu.VMEM((NT, 2 * TILE), BF),
            pltpu.VMEM((ROWS, NT), BF),
            pltpu.VMEM((NT + 16, ROWS), BF),
            pltpu.VMEM((64, NT), BF),
            pltpu.VMEM((NT, 64), BF),
            pltpu.VMEM((BLK_DEV + 16, ROWS), BF),
            pltpu.VMEM((ROWS, BLK_DEV), BF),
            pltpu.VMEM((64, TILE), F32),
            pltpu.VMEM((64, TILE), F32),
            pltpu.VMEM(blocks, F32),
            pltpu.VMEM(blocks, F32),
            pltpu.VMEM(blocks, F32),
            pltpu.VMEM(blocks, F32),
            pltpu.VMEM((1, TILE), F32),
            pltpu.VMEM((1, TILE), F32),
            pltpu.VMEM((ROUNDS * NDEV, MSG, TILE), BF),
            pltpu.VMEM((ROUNDS * NDEV, MSG, TILE), BF),
            pltpu.SemaphoreType.DMA((NT // CHUNK,)),
            pltpu.SemaphoreType.DMA((5,)),
            pltpu.SemaphoreType.DMA((5,)),
            pltpu.SemaphoreType.DMA((ROUNDS,)),
            pltpu.SemaphoreType.DMA((ROUNDS,)),
        ],
        compiler_params=pltpu.CompilerParams(
            collective_id=0, has_side_effects=True, vmem_limit_bytes=60 * 2**20
        ),
    )(
        tiles,
        rays,
        tile_slots.reshape(1, NT),
        tile_rows.reshape(1, NT),
        wanted[0].T,
        tile_count.reshape(1, 1),
    )
    return base + coef_sol * w, vraw * coef_right


def solution(mesh):
    split = Mesh(mesh.devices.reshape(SIZES), AXES)
    placed = (
        P(AXES, None, None),
        P(AXES, None),
        P(AXES),
        P(AXES),
        P(AXES),
        P(AXES, None, None),
    )
    return jax.shard_map(
        per_device,
        mesh=split,
        in_specs=placed,
        out_specs=(P(AXES, None), P(AXES, None)),
        check_vma=False,
    )
```

```python
import jax
import jax.numpy as jnp
from jax import lax
from jax.experimental import pallas as pl
from jax.experimental.pallas import tpu as pltpu
from jax.sharding import Mesh
from jax.sharding import PartitionSpec as P

AXES = ("src_0", "src_1", "reg_0", "reg_1")
SIZES = (4, 4, 4, 2)
NDEV = 128
PEERS = NDEV - 1
BLK_DEV = 256
ITERS = 3
ROUNDS = 2 * ITERS + 2
NT = 512
TILE = 128
GROUP = 128
HALF = GROUP // 2
CHUNK = 32
FLIP = 32
MSG = 4
ROWS = NDEV * MSG
DAMPING = 0.5
BF = jnp.bfloat16
F32 = jnp.float32
MESH = pl.DeviceIdType.MESH


def peers_of(me):
    at = [
        [(me[axis] + off) % SIZES[axis] for off in range(SIZES[axis])] for axis in range(4)
    ]
    offsets = [
        (a, b, c, d) for a in range(4) for b in range(4) for c in range(4) for d in range(2)
    ]
    far = lambda o: -(min(o[0], 4 - o[0]) + min(o[1], 4 - o[1]) + min(o[2], 4 - o[2]) - 0.5 * o[3])
    offsets = sorted((o for o in offsets if any(o)), key=far)
    return [tuple(at[axis][o[axis]] for axis in range(4)) for o in offsets]


def index_of(place):
    return ((place[0] * 4 + place[1]) * 4 + place[2]) * 2 + place[3]


def total(x):
    return jnp.sum(jnp.sum(x, axis=0, keepdims=True), axis=1, keepdims=True)


def low_part(x):
    return x - x.astype(BF).astype(F32)


def kernel(
    tiles_hbm, rays_hbm, slots_hbm, rows_hbm, wanted_hbm, count_hbm,
    base_hbm, w_hbm, vraw_hbm, csol_hbm, cright_hbm,
    tiles, flipped, rays, slots_r, rows_r, wanted_r, count_r,
    picked, parts, s_slot, p_slot, s_row, q_row, comb, gath, uraw_r, u_r, v_r, vraw_r, w_r, sol_r, csol_r, cright_r,
    send, recv, load_sem, small_sem, out_sem, send_sem, recv_sem,
):
    me = tuple(lax.axis_index(axis) for axis in AXES)
    mine = index_of(me)
    others = peers_of(me)

    smalls = [
        pltpu.make_async_copy(src, dst, small_sem.at[i])
        for i, (src, dst) in enumerate(
            [
                (rows_hbm, rows_r),
                (rays_hbm, rays),
                (slots_hbm, slots_r),
                (count_hbm, count_r),
                (wanted_hbm, wanted_r),
            ]
        )
    ]

    def load(g):
        at = pl.ds(g * CHUNK, CHUNK)
        return pltpu.make_async_copy(tiles_hbm.at[at], tiles.at[at], load_sem.at[g])

    for copy in smalls:
        copy.start()
    for g in range(NT // CHUNK):
        load(g).start()
    barrier = pltpu.get_barrier_semaphore()
    for place in others:
        pl.semaphore_signal(barrier, inc=1, device_id=place, device_id_type=MESH)

    iota = lambda shape, dim: lax.broadcasted_iota(jnp.int32, shape, dim)
    zero = jnp.zeros((), BF)
    msg_id = iota((ROWS, TILE), 0) % MSG
    diag = (iota((GROUP, HALF * TILE), 0) % HALF) == (iota((GROUP, HALF * TILE), 1) // TILE)

    def one_hot(left, right):
        return jnp.where(left == right, 1.0, 0.0).astype(BF)

    def start_round(r, data, square):
        message = jnp.where(msg_id == 2, square, jnp.where(msg_id == 3, low_part(square), data))
        at = pl.ds(pl.multiple_of(r * ROWS, ROWS), ROWS)
        send.reshape(ROUNDS * ROWS, TILE)[at, :] = message.astype(BF)
        recv[r * NDEV + mine] = send[r * NDEV + mine]
        for place in others:
            pltpu.make_async_remote_copy(
                src_ref=send.at[r * NDEV + index_of(place)],
                dst_ref=recv.at[r * NDEV + mine],
                send_sem=send_sem.at[r],
                recv_sem=recv_sem.at[r],
                device_id=place,
                device_id_type=MESH,
            ).start()

    def end_round(r):
        landed = recv.at[pl.ds(r * NDEV, PEERS)]
        pltpu.make_async_copy(landed, landed, recv_sem.at[r]).wait()
        at = pl.ds(pl.multiple_of(r * ROWS, ROWS), ROWS)
        return recv.reshape(ROUNDS * ROWS, TILE)[at, :]

    def tile_group(source, g):
        at = g * GROUP
        lhs = jnp.where(diag, jnp.tile(picked[pl.ds(at, GROUP), :], (1, HALF)), zero)
        pair = [source[pl.ds(at + HALF * h, HALF)].reshape(HALF * TILE, TILE) for h in range(2)]
        result = jnp.dot(lhs, jnp.concatenate(pair, axis=1), preferred_element_type=F32)
        for h, part in enumerate((result[:HALF, :TILE], result[HALF:, TILE:])):
            where = pl.ds(at + HALF * h, HALF)
            parts[where, :TILE] = part.astype(BF)
            parts[where, TILE:] = low_part(part).astype(BF)

    def flip(first, count):
        def step(i, c):
            at = first + i * FLIP
            for j in range(FLIP):
                flipped[at + j] = tiles[at + j].T
            return c

        lax.fori_loop(0, count // FLIP, step, 0)

    def pick_rays(uraw):
        picked[...] = jnp.dot(q_row[...], uraw.astype(BF), preferred_element_type=F32).astype(BF)

    def both_halves(selector):
        sums = jnp.dot(selector, parts[...], preferred_element_type=F32)
        return sums[:, :TILE] + sums[:, TILE:]

    def owner_vraw(r, v):
        both = jnp.dot(comb[...], end_round(r), preferred_element_type=F32)
        beta = jnp.sqrt(both[:1, :])
        return beta, both[16:, :] / beta - beta * v

    smalls[0].wait()
    s_row[...] = one_hot(iota((64, NT), 0), rows_r[...])
    q_row[...] = one_hot(iota((64, NT), 0), rows_r[...]).astype(F32).T.astype(BF)
    smalls[1].wait()
    uraw = rays[...]
    uraw_r[...] = uraw
    pick_rays(uraw)
    smalls[2].wait()
    smalls[3].wait()
    target = jnp.where(msg_id < 2, (iota((ROWS, TILE), 0) // MSG) * 2 + msg_id, -1)
    live_slots = jnp.where(iota((1, NT), 1) < count_r[...], slots_r[...], -2)
    for j in range(NT // TILE):
        s_slot[:, j * TILE : (j + 1) * TILE] = one_hot(
            target, live_slots[:, j * TILE : (j + 1) * TILE]
        )
    v_r[...] = jnp.zeros_like(v_r)
    w_r[...] = jnp.zeros_like(w_r)
    sol_r[...] = jnp.zeros_like(sol_r)
    square = total(uraw * uraw)
    per_group = GROUP // CHUNK
    for g in range(NT // GROUP):
        for c in range(per_group):
            load(g * per_group + c).wait()
        tile_group(tiles, g)
    sums = both_halves(s_slot[...])
    pl.semaphore_wait(barrier, PEERS)
    start_round(0, sums, square)

    smalls[4].wait()
    asked = jnp.concatenate([wanted_r[0:1, :], wanted_r[1:2, :]], axis=1)
    owned = one_hot(iota((BLK_DEV, 2 * NDEV), 0), asked)
    row = iota((ROWS, 2 * NDEV), 0)
    place_of = jnp.where(row % MSG < 2, (row % MSG) * NDEV + row // MSG, -1)
    spread = one_hot(place_of, iota((ROWS, 2 * NDEV), 1))
    nt = (((1,), (1,)), ((), ()))
    comb[16:, :] = lax.dot_general(
        owned, spread, nt, preferred_element_type=F32
    ).astype(BF)
    gath[...] = lax.dot_general(spread, owned, nt, preferred_element_type=F32).astype(BF)
    scalar_rows = jnp.logical_and(iota((16, ROWS), 0) == 0, iota((16, ROWS), 1) % MSG >= 2)
    scalar_rows = jnp.where(scalar_rows, 1.0, 0.0).astype(BF)
    comb[:16, :] = scalar_rows
    flip(0, NT // 2)

    def iteration(k, carry):
        phibar, rhobar = carry
        beta, vraw = owner_vraw(2 * k, v_r[...])
        outgoing = jnp.dot(gath[...], vraw.astype(BF), preferred_element_type=F32)
        start_round(2 * k + 1, outgoing, total(vraw * vraw))
        vraw_r[...] = vraw
        u_r[...] = uraw_r[...] / beta

        @pl.when(k == 0)
        def _():
            p_slot[:NT, :] = s_slot[...].T
            p_slot[NT:, :] = scalar_rows
            flip(NT // 2, NT // 2)

        both = jnp.dot(p_slot[...], end_round(2 * k + 1), preferred_element_type=F32)
        alpha = jnp.sqrt(both[NT : NT + 1, :])
        picked[...] = both[:NT, :].astype(BF)
        for g in range(NT // GROUP):
            tile_group(flipped, g)
        uraw = both_halves(s_row[...]) / alpha - alpha * u_r[...]
        uraw_r[...] = uraw
        pick_rays(uraw)
        for g in range(NT // GROUP):
            tile_group(tiles, g)
        start_round(2 * k + 2, both_halves(s_slot[...]), total(uraw * uraw))

        first = k == 0
        v_new = vraw_r[...] / alpha
        rhobar1 = jnp.sqrt(rhobar * rhobar + DAMPING * DAMPING)
        phibar = rhobar / rhobar1 * phibar
        rho = jnp.sqrt(rhobar1 * rhobar1 + beta * beta)
        cosine = rhobar1 / rho
        sine = beta / rho
        theta = sine * alpha
        w = w_r[...]
        sol_r[...] += jnp.where(first, 0.0, cosine * phibar / rho) * w
        w_r[...] = v_new - jnp.where(first, 0.0, theta / rho) * w
        v_r[...] = v_new
        phibar = jnp.where(first, beta, sine * phibar)
        rhobar = jnp.where(first, alpha, -cosine * alpha)
        return phibar, rhobar

    nothing = jnp.zeros((1, TILE), F32)
    phibar, rhobar = lax.fori_loop(0, ITERS, iteration, (nothing, nothing))

    outs = [
        pltpu.make_async_copy(src, dst, out_sem.at[i])
        for i, (src, dst) in enumerate(
            [(sol_r, base_hbm), (w_r, w_hbm), (vraw_r, vraw_hbm), (csol_r, csol_hbm), (cright_r, cright_hbm)]
        )
    ]
    outs[0].start()
    outs[1].start()
    beta, vraw = owner_vraw(2 * ITERS, v_r[...])
    start_round(2 * ITERS + 1, jnp.zeros((ROWS, TILE), F32), total(vraw * vraw))
    vraw_r[...] = vraw
    outs[2].start()
    rhobar1 = jnp.sqrt(rhobar * rhobar + DAMPING * DAMPING)
    phibar = rhobar / rhobar1 * phibar
    rho = jnp.sqrt(rhobar1 * rhobar1 + beta * beta)
    csol_r[...] = rhobar1 / rho * phibar / rho
    outs[3].start()

    def drain(r, c):
        sent = send.at[pl.ds(r * NDEV, PEERS)]
        pltpu.make_async_copy(sent, sent, send_sem.at[r]).wait()
        return c

    lax.fori_loop(0, ROUNDS, drain, 0)
    for copy in outs[:4]:
        copy.wait()
    both = jnp.dot(comb[:16, :], end_round(2 * ITERS + 1), preferred_element_type=F32)
    cright_r[...] = (BLK_DEV * TILE * NDEV) ** 0.5 / jnp.sqrt(both[0:1, :])
    outs[4].start()
    outs[4].wait()


def per_device(tiles, rays, tile_rows, tile_slots, tile_count, wanted):
    hbm = pl.BlockSpec(memory_space=pltpu.HBM)
    blocks = (BLK_DEV, TILE)
    shapes = [blocks, blocks, blocks, (1, TILE), (1, TILE)]
    base, w, vraw, coef_sol, coef_right = pl.pallas_call(
        kernel,
        name="lsqr",
        out_shape=[jax.ShapeDtypeStruct(shape, F32) for shape in shapes],
        in_specs=[hbm] * 6,
        out_specs=[hbm] * 5,
        scratch_shapes=[
            pltpu.VMEM((NT, TILE, TILE), BF),
            pltpu.VMEM((NT, TILE, TILE), BF),
            pltpu.VMEM((64, TILE), F32),
            pltpu.VMEM((1, NT), jnp.int32),
            pltpu.VMEM((1, NT), jnp.int32),
            pltpu.VMEM((2, NDEV), jnp.int32),
            pltpu.VMEM((1, 1), jnp.int32),
            pltpu.VMEM((NT, TILE), BF),
            pltpu.VMEM((NT, 2 * TILE), BF),
            pltpu.VMEM((ROWS, NT), BF),
            pltpu.VMEM((NT + 16, ROWS), BF),
            pltpu.VMEM((64, NT), BF),
            pltpu.VMEM((NT, 64), BF),
            pltpu.VMEM((BLK_DEV + 16, ROWS), BF),
            pltpu.VMEM((ROWS, BLK_DEV), BF),
            pltpu.VMEM((64, TILE), F32),
            pltpu.VMEM((64, TILE), F32),
            pltpu.VMEM(blocks, F32),
            pltpu.VMEM(blocks, F32),
            pltpu.VMEM(blocks, F32),
            pltpu.VMEM(blocks, F32),
            pltpu.VMEM((1, TILE), F32),
            pltpu.VMEM((1, TILE), F32),
            pltpu.VMEM((ROUNDS * NDEV, MSG, TILE), BF),
            pltpu.VMEM((ROUNDS * NDEV, MSG, TILE), BF),
            pltpu.SemaphoreType.DMA((NT // CHUNK,)),
            pltpu.SemaphoreType.DMA((5,)),
            pltpu.SemaphoreType.DMA((5,)),
            pltpu.SemaphoreType.DMA((ROUNDS,)),
            pltpu.SemaphoreType.DMA((ROUNDS,)),
        ],
        compiler_params=pltpu.CompilerParams(
            collective_id=0, has_side_effects=True, vmem_limit_bytes=60 * 2**20
        ),
    )(
        tiles,
        rays,
        tile_slots.reshape(1, NT),
        tile_rows.reshape(1, NT),
        wanted[0].T,
        tile_count.reshape(1, 1),
    )
    return base + coef_sol * w, vraw * coef_right


def solution(mesh):
    split = Mesh(mesh.devices.reshape(SIZES), AXES)
    placed = (
        P(AXES, None, None),
        P(AXES, None),
        P(AXES),
        P(AXES),
        P(AXES),
        P(AXES, None, None),
    )
    return jax.shard_map(
        per_device,
        mesh=split,
        in_specs=placed,
        out_specs=(P(AXES, None), P(AXES, None)),
        check_vma=False,
    )
```
